32 devices in a mesh: pix: 8 (over y, x, core), tm: 4 (over z).
Axes of the slice: x: 2, y: 2, z: 4, core: 2. Of those that a mesh axis runs over, the one named last changes fastest.
Arguments:
- recording: bfloat16 [128, 256, 512], P('pix', None, 'tm'), may hold values from 0 to 12, as said below
- footprints: float32 [128, 2, 256, 128], P('pix'), may hold values from 0 to 0.03
- traces: float32 [96, 128, 512], P(None, None, 'tm'), may hold values from 0 to 1
- block_list: int32 [128, 2], P('pix'), may hold values from 0 to 95, as said below
- block_order: int32 [96], replicated, may hold values from 0 to 95, as said below
Outputs:
- footprints_out: float32 [128, 2, 256, 128], P('pix')
- traces_out: float32 [96, 128, 512], P(None, None, 'tm')
The draws below stay inside these ranges and needn't reach their ends.
Inputs may be any that keep to these rules, and one draw needn't show every extreme that they name: `recording`: nonnegative intensities. block_list[p, g] is one of block_order[g * 48] to block_order[(g + 1) * 48 - 1], and every block is named by some patch. `block_order`: a permutation of the component blocks.
All inputs are finite; a program needn't handle non-finite values.
Results may differ from the reference program's by a relative error of at most 0.0003.
Values sent between devices are 32-bit elements; how exact they have to be, the bound alone decides.
No kernel may reach another device: no remote copies, remote signals or barrier semaphores. Data moves between devices by JAX's collectives and lax.ppermute only.
A program may use at most 128 MiB of HBM per device.

```python
import jax
import jax.numpy as jnp
from jax import lax

PATCH = 256
KB = 128
GROUPS = 2
BPG = 48
SWEEPS = 2
BLOCKS = 96
PATCHES = 128
FRAMES = 512


def block_tables(key):
    order = jax.random.permutation(jax.random.fold_in(key, 7), BLOCKS).astype(jnp.int32)
    columns = []
    for group_index in range(GROUPS):
        spread = jax.random.permutation(jax.random.fold_in(key, 11 + group_index), PATCHES).astype(jnp.int32) % BPG
        columns.append(order[group_index * BPG + spread])
    return (order, jnp.stack(columns, axis=1).astype(jnp.int32))


def draw_block_list(key, part):
    order, listing = block_tables(key)
    return listing


def draw_block_order(key, part):
    order, listing = block_tables(key)
    return order


def draw_recording(key, part):
    position = jnp.arange(FRAMES, dtype=jnp.float32) / (FRAMES - 1)
    values = jax.random.uniform(jax.random.fold_in(key, 31), (PATCHES, PATCH, FRAMES), jnp.float32, 0.0, 4.0)
    rising = 1.0 + 2.0 * position
    return (values * rising[None, None, :]).astype(jnp.bfloat16)


def level_of(own_key, extent, shards, smallest, largest):
    factor_of, own = 1.0, jax.random.fold_in(own_key, 6)
    for axis_at, shards_of in shards:
        steps = jnp.exp(jax.random.uniform(jax.random.fold_in(own, axis_at), (shards_of,), jnp.float32, smallest / len(shards), largest / len(shards)))
        factor_of = factor_of * jnp.repeat(steps, extent[axis_at] // shards_of).reshape([-1 if axis == axis_at else 1 for axis in range(len(extent))])
    return factor_of


def setup_inputs(seed: int = 0) -> dict:
    arg_keys = jax.random.split(jax.random.key(seed), 6)
    recording = draw_recording(jax.random.fold_in(arg_keys[5], 71), 0)
    footprints = jnp.clip(0.03 * jax.random.uniform(arg_keys[1], (PATCHES, GROUPS, PATCH, KB), jnp.float32) ** level_of(arg_keys[1], (PATCHES, GROUPS, PATCH, KB), ((0, 8),), -0.2, 0.2), 0.0, 0.03)
    traces = jnp.clip(1.0 * jax.random.uniform(arg_keys[2], (BLOCKS, KB, FRAMES), jnp.float32) ** level_of(arg_keys[2], (BLOCKS, KB, FRAMES), ((2, 4),), -0.2, 0.2), 0.0, 1.0)
    block_list = draw_block_list(jax.random.fold_in(arg_keys[5], 71), 0)
    block_order = draw_block_order(jax.random.fold_in(arg_keys[5], 71), 0)
    return dict(recording=recording, footprints=footprints, traces=traces, block_list=block_list, block_order=block_order)


epsilon = 1e-6


def product(form, left, right):
    return jnp.einsum(form, left, right, precision=lax.Precision.HIGHEST)


def member_table(block_list, block_order, group_index):
    chosen = block_order[group_index * BPG:(group_index + 1) * BPG]
    member = (block_list[:, group_index][:, None] == chosen[None, :]).astype(jnp.float32)
    return member, chosen


def reference(recording, footprints, traces, block_list, block_order):
    residual = recording.astype(jnp.float32)
    for group_index in range(GROUPS):
        current = jnp.take(traces, block_list[:, group_index], axis=0)
        residual = residual - product("pvk,pkf->pvf", footprints[:, group_index], current)
    for sweep_index in range(SWEEPS):
        norms = []
        for group_index in range(GROUPS):
            member, chosen = member_table(block_list, block_order, group_index)
            squares = jnp.sum(footprints[:, group_index] * footprints[:, group_index], axis=1)
            norms.append(product("pj,pk->jk", member, squares))
        for group_index in range(GROUPS):
            member, chosen = member_table(block_list, block_order, group_index)
            local_terms = product("pvk,pvf->pkf", footprints[:, group_index], residual)
            totals = product("pj,pkf->jkf", member, local_terms)
            before = jnp.take(traces, chosen, axis=0)
            after = jnp.maximum(before + totals / (KB * norms[group_index][:, :, None] + epsilon), 0.0)
            traces = traces.at[chosen].set(after)
            change = product("pj,jkf->pkf", member, after - before)
            residual = residual - product("pvk,pkf->pvf", footprints[:, group_index], change)
        energy = jnp.sum(traces * traces, axis=2)
        for group_index in range(GROUPS):
            current = jnp.take(traces, block_list[:, group_index], axis=0)
            weights = product("pvf,pkf->pvk", residual, current)
            scale = jnp.take(energy, block_list[:, group_index], axis=0)
            previous = footprints[:, group_index]
            updated = jnp.maximum(previous + weights / (KB * scale[:, None, :] + epsilon), 0.0)
            footprints = footprints.at[:, group_index].set(updated)
            residual = residual - product("pvk,pkf->pvf", updated - previous, current)
    return footprints, traces
```

```python
import functools

import jax
import jax.numpy as jnp
from jax import lax
from jax.experimental import pallas as pl
from jax.experimental.pallas import tpu as pltpu
from jax.sharding import PartitionSpec as P


EPSILON = 1e-06
SUBLANES = 8
f32 = jnp.float32
bf16 = jnp.bfloat16


def up8(n):
    return -(-n // SUBLANES) * SUBLANES


def divisor(n, limits):
    return max(m for m in limits if n % m == 0)


def split(x):
    high = x.astype(bf16)
    return high, (x - high.astype(f32)).astype(bf16)


def dot(a, b, ca, cb):
    return lax.dot_general(a, b, (((ca,), (cb,)), ((), ())), preferred_element_type=f32)


def rows_by_rows(a, b):
    left = jnp.concatenate(a, axis=1)
    right = jnp.concatenate([b[0], b[0]], axis=1)
    return dot(left, right, 1, 1) + dot(a[0], b[1], 1, 1)


def rows_by_columns(a, b, ca=1):
    n = b[0].shape[1]
    both = dot(a[0], jnp.concatenate(b, axis=1), ca, 0)
    return both[:, :n] + both[:, n:] + dot(a[1], b[0], ca, 0)


def full_spec(shape):
    return pl.BlockSpec(shape, lambda *_: (0,) * len(shape))


def squares(x):
    return jnp.sum(x * x, axis=0, keepdims=True)


def first_kernel(bl, y, foot, *refs, parts, own, step):
    t0s, t1s = refs[:step], refs[step:2 * step]
    pos, base_out, pay = refs[2 * step:]
    at = pl.program_id(0) * step
    count = pl.num_programs(0) * step
    kb = foot.shape[3]
    for i in range(step):
        f0, f1 = split(foot[i, 0]), split(foot[i, 1])
        base = y[i].astype(f32) - rows_by_columns(f1, split(t1s[i][0]))
        base_out[i] = base
        residual = base - rows_by_columns(f0, split(t0s[i][0]))
        terms = rows_by_columns(split(residual), f0, 0)
        p = at + i
        pay[:, pl.ds(pl.multiple_of(p * own, SUBLANES), own), :] = terms.reshape(parts, own, kb)
        for g in range(2):
            norm = jnp.broadcast_to(squares(foot[i, g])[None], (parts, 1, kb))
            pay[:, pl.ds(count * own + g * count + p, 1), :] = norm

    @pl.when(at == 0)
    def _():
        start = pay.shape[1] - pos.shape[0]
        pay[:, start:, :] = jnp.broadcast_to(pos[...][None], (parts,) + pos.shape)


def second_kernel(base, foot, rx, pay, *, parts, own, step):
    at = pl.program_id(0) * step
    kb = foot.shape[3]
    for i in range(step):
        f0, f1 = split(foot[i, 0]), split(foot[i, 1])
        trace = rx[:, i].reshape(parts * own, kb)
        residual = base[i] - rows_by_rows(f0, split(trace))
        terms = rows_by_columns(split(residual), f1, 0)
        pay[:, pl.ds(pl.multiple_of((at + i) * own, SUBLANES), own), :] = terms.reshape(parts, own, kb)


def prepare_kernel(order, pix, *refs, own, step):
    ins, out, flipped = refs[:step], refs[step], refs[step + 1]
    for i in range(step):
        flipped[i] = ins[i][0].T
        out[i] = flipped[i, pl.ds(pl.multiple_of(pix[0] * own, SUBLANES), own), :]


def owner_kernel(listing, place, order, rx, before, *refs, group, per, own, outs, outper, other):
    if other == "norms":
        after, back, norms1, totals, norms = refs
        norms1[...] = jnp.zeros(norms1.shape, f32)
        norms[...] = jnp.zeros(norms.shape, f32)
    elif other == "final":
        norms, after0, after, back, final, totals = refs
    else:
        norms, after, back, totals = refs
    sources = rx.shape[0]
    kb = rx.shape[2]
    bpg = before.shape[0]
    totals[...] = jnp.zeros(totals.shape, f32)

    @pl.loop(0, sources)
    def _(s):
        for i in range(per):
            p = s * per + i
            j = place[listing[p, group]] - group * bpg
            totals[j] = totals[j] + rx[s, i * own:(i + 1) * own, :]
            if other == "norms":
                row = per * own + i
                norms[j] = norms[j] + jnp.broadcast_to(rx[s, row:row + 1, :], (SUBLANES, kb))
                j1 = place[listing[p, 1]] - bpg
                row = per * own + per + i
                norms1[j1] = norms1[j1] + jnp.broadcast_to(rx[s, row:row + 1, :], (SUBLANES, kb))

    scale = kb * norms[:, 0:1, :] + EPSILON
    after[...] = jnp.maximum(before[...] + totals[...] / scale, 0.0)

    @pl.loop(0, outs)
    def _(s):
        for i in range(outper):
            j = place[listing[s * outper + i, group]] - group * bpg
            back[s, i * own:(i + 1) * own, :] = after[j]

    if other == "final":

        @pl.loop(0, bpg, unroll=4)
        def _(j):
            final[order[j]] = after0[j]
            final[order[bpg + j]] = after[j]


def owner(tables, rx, before, extra, *, group, per, outs, outper, other):
    bpg, own, kb = before.shape
    norms_shape = (bpg, SUBLANES, kb)
    shapes = [before.shape, (outs, outper * own, kb)]
    if other == "norms":
        shapes.append(norms_shape)
    if other == "final":
        shapes.append((2 * bpg, own, kb))
    scratch = [pltpu.VMEM(before.shape, f32)]
    if other == "norms":
        scratch.append(pltpu.VMEM(norms_shape, f32))
    return pl.pallas_call(
        functools.partial(owner_kernel, group=group, per=per, own=own, outs=outs, outper=outper, other=other),
        grid_spec=pltpu.PrefetchScalarGridSpec(
            num_scalar_prefetch=3,
            grid=(1,),
            in_specs=[full_spec(x.shape) for x in (rx, before, *extra)],
            out_specs=[full_spec(shape) for shape in shapes],
            scratch_shapes=scratch,
        ),
        out_shape=[jax.ShapeDtypeStruct(shape, f32) for shape in shapes],
        name="owner",
    )(*tables, rx, before, *extra)


def incoming(rx, i, me, ntm):
    pieces = []
    for s in range(ntm):
        piece = rx[:, lax.rem(me + (ntm - s), ntm), i]
        pieces.append(piece.reshape(piece.shape[0] * piece.shape[1], piece.shape[2]))
    return jnp.concatenate(pieces, axis=0)


def outgoing(pay, terms, p, me, ntm):
    npix, kb = pay.shape[0], terms.shape[1]
    own = terms.shape[0] // (npix * ntm)
    for s in range(ntm):
        piece = terms[s * npix * own:(s + 1) * npix * own].reshape(npix, own, kb)
        to = lax.rem(me + (ntm - s), ntm)
        pay[:, to, pl.ds(pl.multiple_of(p * own, SUBLANES), own), :] = piece


def footprint_phase(residual, f0, f1, t0, t1):
    kb = f0.shape[1]
    scale0 = kb * squares(t0) + EPSILON
    scale1 = kb * squares(t1) + EPSILON
    s0, s1 = split(t0), split(t1)
    n0 = jnp.maximum(f0 + rows_by_columns(split(residual), s0) / scale0, 0.0)
    residual = residual - rows_by_rows(split(n0 - f0), s0)
    n1 = jnp.maximum(f1 + rows_by_columns(split(residual), s1) / scale1, 0.0)
    return residual, n0, n1, s1


def merge_kernel(me_ref, *refs, ntm, step):
    ys, t0s = refs[:ntm], refs[ntm:2 * ntm]
    foot, residual_out, t0_out = refs[2 * ntm:]
    kb = foot.shape[3]
    for i in range(step):
        y = jnp.concatenate([ref[i] for ref in ys], axis=1)
        t0 = jnp.concatenate([ref[:, i].reshape(ref.shape[0] * ref.shape[2], kb) for ref in t0s], axis=0)
        residual_out[i] = y - rows_by_rows(split(foot[i, 0]), split(t0))
        t0_out[i] = t0


def third_kernel(me_ref, part, t0_in, rx1, foot, residual_out, foot_out, t1_out, pay, *, ntm, step):
    me = me_ref[0]
    at = pl.program_id(0) * step
    count = pl.num_programs(0) * step
    for i in range(step):
        f0, f1 = foot[i, 0], foot[i, 1]
        t1 = incoming(rx1, i, me, ntm)
        residual = part[i] - rows_by_rows(split(f1), split(t1))
        residual, n0, n1, s1 = footprint_phase(residual, f0, f1, t0_in[i], t1)
        residual = residual - rows_by_rows(split(n1 - f1), s1)
        residual_out[i] = residual
        foot_out[i, 0] = n0
        foot_out[i, 1] = n1
        t1_out[i] = t1
        outgoing(pay, rows_by_columns(split(residual), split(n0), 0), at + i, me, ntm)
        own = (pay.shape[2] - up8(2 * count)) // count
        for g, new in enumerate((n0, n1)):
            norm = jnp.broadcast_to(squares(new)[None, None], pay.shape[:2] + (1, new.shape[1]))
            pay[:, :, pl.ds(count * own + g * count + at + i, 1), :] = norm


def ahead_kernel(residual, foot, terms_out, gram_out, *, step):
    for i in range(step):
        f1 = split(foot[i, 1])
        terms_out[i] = rows_by_columns(split(residual[i]), f1, 0)
        gram_out[i] = rows_by_columns(split(foot[i, 0]), f1, 0)


def fourth_kernel(me_ref, terms, gram, told, rx, change_out, pay, *, ntm, step):
    me = me_ref[0]
    at = pl.program_id(0) * step
    for i in range(step):
        change = incoming(rx, i, me, ntm) - told[i]
        change_out[i] = change
        new = terms[i] - rows_by_columns(split(change), split(gram[i]))
        outgoing(pay, new, at + i, me, ntm)


def late_kernel(residual, foot, change, residual_out, *, step):
    for i in range(step):
        residual_out[i] = residual[i] - rows_by_rows(split(foot[i, 0]), split(change[i]))


def last_kernel(me_ref, residual_in, foot, told, rx0, rx1, foot_out, *, ntm, step):
    me = me_ref[0]
    for i in range(step):
        f0, f1 = foot[i, 0], foot[i, 1]
        t0 = incoming(rx0, i, me, ntm)
        t1 = incoming(rx1, i, me, ntm)
        residual = residual_in[i] - rows_by_rows(split(f1), split(t1 - told[i]))
        _, n0, n1, _ = footprint_phase(residual, f0, f1, t0, t1)
        foot_out[i, 0] = n0
        foot_out[i, 1] = n1


def flip_kernel(rx, out):
    npix, count, own, kb = rx.shape
    for j in range(count):
        out[j] = rx[:, j].reshape(npix * own, kb).T


def line_gather(chunks, axis, n):
    me = lax.axis_index(axis)
    size = sum(x.shape[0] for x in chunks)
    rest = chunks[0].shape[1:]
    left, right = list(chunks), list(chunks)
    from_left, from_right = {}, {}
    for s in range(1, n):
        for c in range(len(chunks)):
            left[c] = lax.ppermute(left[c], axis, [(j, j + 1) for j in range(n - 1)])
            right[c] = lax.ppermute(right[c], axis, [(j, j - 1) for j in range(1, n)])
            from_left[s, c], from_right[s, c] = left[c], right[c]
    out = jnp.zeros((n * size,) + rest, chunks[0].dtype)
    offset = 0
    for c, x in enumerate(chunks):
        out = lax.dynamic_update_slice_in_dim(out, x, me * size + offset, 0)
        for s in range(1, n):
            piece = jnp.where(me + s < n, from_right[s, c], from_left[n - s, c])
            out = lax.dynamic_update_slice_in_dim(out, piece, lax.rem(me + s, n) * size + offset, 0)
        offset += x.shape[0]
    return out


def local(recording, footprints, traces, block_list, block_order, *, npix, ntm):
    count, voxels, frames = recording.shape
    groups, kb = footprints.shape[1], footprints.shape[3]
    blocks = traces.shape[0]
    bpg = blocks // groups
    own = frames // npix
    share = count // ntm
    everyone = npix * ntm
    every = frames * ntm
    pix, tm = lax.axis_index("pix"), lax.axis_index("tm")
    me = jnp.reshape(tm, (1,)).astype(jnp.int32)

    def kernel(body, grid, in_specs, out_specs, out_shape, prefetch=0, scratch=(), **static):
        return pl.pallas_call(
            functools.partial(body, **static),
            grid_spec=pltpu.PrefetchScalarGridSpec(
                num_scalar_prefetch=prefetch,
                grid=grid,
                in_specs=in_specs,
                out_specs=out_specs,
                scratch_shapes=scratch,
            ),
            out_shape=out_shape,
        )

    def array(*shape):
        return jax.ShapeDtypeStruct(shape, f32)

    def exchange(x, axes):
        return lax.all_to_all(x, axes, 0, 0, tiled=True)

    y_pieces = []
    for s in range(ntm):
        to = lax.rem(tm + s, ntm)
        piece = lax.dynamic_slice_in_dim(recording, to * share, share, 0).astype(f32)
        y_pieces.append(lax.ppermute(piece, "tm", [(j, (j + s) % ntm) for j in range(ntm)]) if s else piece)

    pos_rows = up8(-(-count * groups // kb))
    pos_row = jnp.pad(
        block_list.astype(f32).reshape(-1), (0, pos_rows * kb - count * groups)
    ).reshape(pos_rows, kb)
    place = jnp.zeros((blocks,), jnp.int32).at[block_order].set(jnp.arange(blocks, dtype=jnp.int32))

    step = divisor(count, (4, 2, 1))
    rows = count * own + up8(groups * count)
    foot_spec = pl.BlockSpec((step, groups, voxels, kb), lambda p, *_: (p, 0, 0, 0))
    patch_spec = pl.BlockSpec((step, voxels, frames), lambda p, *_: (p, 0, 0))

    def block_spec(i, g):
        return pl.BlockSpec((1, kb, frames), lambda p, bl: (bl[p * step + i, g], 0, 0))

    base, pay = kernel(
        first_kernel, (count // step,),
        [patch_spec, foot_spec] + [block_spec(i, g) for g in range(groups) for i in range(step)]
        + [full_spec(pos_row.shape)],
        [patch_spec, full_spec((npix, rows + pos_rows, kb))],
        [array(count, voxels, frames), array(npix, rows + pos_rows, kb)],
        prefetch=1, parts=npix, own=own, step=step,
    )(block_list, recording, footprints, *[traces] * (groups * step), pos_row)
    got = exchange(pay, "pix")

    several = divisor(bpg, (8, 4, 2, 1))
    whereabouts = jnp.reshape(pix, (1,)).astype(jnp.int32)

    def prepared(g):
        def ordered_spec(i):
            return pl.BlockSpec(
                (1, kb, frames), lambda b, order, pix: (order[g * bpg + b * several + i], 0, 0)
            )

        return kernel(
            prepare_kernel, (bpg // several,),
            [ordered_spec(i) for i in range(several)],
            pl.BlockSpec((several, own, kb), lambda b, *_: (b, 0, 0)),
            array(bpg, own, kb),
            prefetch=2, scratch=[pltpu.VMEM((several, frames, kb), f32)], own=own, step=several,
        )(block_order, whereabouts, *[traces] * several)

    before0, before1 = prepared(0), prepared(1)

    listing = got[:, rows:, :].reshape(npix, -1)[:, :count * groups].reshape(npix * count, groups)
    tables = (listing.astype(jnp.int32), place, block_order)
    after0, back, norms1 = owner(
        tables, got, before0, (), group=0, per=count, outs=npix, outper=count, other="norms"
    )
    rx0 = exchange(back, "pix").reshape(npix, count, own, kb)

    t0_pieces = []
    for s in range(ntm):
        to = lax.rem(tm + s, ntm)
        piece = lax.dynamic_slice_in_dim(rx0, to * share, share, 1)
        t0_pieces.append(lax.ppermute(piece, "tm", [(j, (j + s) % ntm) for j in range(ntm)]) if s else piece)

    pay = kernel(
        second_kernel, (count // step,),
        [patch_spec, foot_spec, pl.BlockSpec((npix, step, own, kb), lambda p: (0, p, 0, 0))],
        full_spec((npix, count * own, kb)),
        array(npix, count * own, kb),
        parts=npix, own=own, step=step,
    )(base, footprints, rx0)
    after1, back = owner(
        tables, exchange(pay, "pix"), before1, (norms1,),
        group=1, per=count, outs=everyone, outper=share, other=None,
    )

    def spread(x):
        return exchange(x.reshape(everyone, x.shape[-2], kb), ("pix", "tm"))

    def landed(x):
        return x.reshape(npix, ntm, share, own, kb)

    rx1 = landed(spread(back))

    step = divisor(share, (2, 1))
    grid = (share // step,)
    share_spec = pl.BlockSpec((step, voxels, frames), lambda p, *_: (p, 0, 0))
    part_spec = pl.BlockSpec((npix, step, own, kb), lambda p, *_: (0, p, 0, 0))
    rx_spec = pl.BlockSpec((npix, ntm, step, own, kb), lambda p, *_: (0, 0, p, 0, 0))
    residual_spec = pl.BlockSpec((step, voxels, every), lambda p, *_: (p, 0, 0))
    trace_spec = pl.BlockSpec((step, every, kb), lambda p, *_: (p, 0, 0))
    gram_spec = pl.BlockSpec((step, kb, kb), lambda p, *_: (p, 0, 0))
    foot_spec = pl.BlockSpec((step, groups, voxels, kb), lambda p, *_: (p, 0, 0, 0))
    own_foot_spec = pl.BlockSpec(
        (step, groups, voxels, kb), lambda p, me: (me[0] * (share // step) + p, 0, 0, 0)
    )
    residual_type, trace_type = array(share, voxels, every), array(share, every, kb)
    foot_type = array(share, groups, voxels, kb)
    wide = (npix, ntm, share * own + up8(groups * share), kb)
    narrow = (npix, ntm, share * own, kb)

    part, t0_old = kernel(
        merge_kernel, grid,
        [share_spec] * ntm + [part_spec] * ntm + [own_foot_spec],
        [residual_spec, trace_spec],
        [residual_type, trace_type],
        prefetch=1, ntm=ntm, step=step,
    )(me, *y_pieces, *t0_pieces, footprints)
    residual, foot, t1_old, pay = kernel(
        third_kernel, grid,
        [residual_spec, trace_spec, rx_spec, own_foot_spec],
        [residual_spec, foot_spec, trace_spec, full_spec(wide)],
        [residual_type, foot_type, trace_type, array(*wide)],
        prefetch=1, ntm=ntm, step=step,
    )(me, part, t0_old, rx1, footprints)

    got = spread(pay)
    terms, gram = kernel(
        ahead_kernel, grid,
        [residual_spec, foot_spec],
        [trace_spec, gram_spec],
        [trace_type, array(share, kb, kb)],
        step=step,
    )(residual, foot)
    after0, back, norms1 = owner(
        tables, got, after0, (), group=0, per=share, outs=everyone, outper=share, other="norms"
    )
    rx0 = landed(spread(back))
    change, pay = kernel(
        fourth_kernel, grid,
        [trace_spec, gram_spec, trace_spec, rx_spec],
        [trace_spec, full_spec(narrow)],
        [trace_type, array(*narrow)],
        prefetch=1, ntm=ntm, step=step,
    )(me, terms, gram, t0_old, rx0)
    got = spread(pay)
    residual = kernel(
        late_kernel, grid,
        [residual_spec, foot_spec, trace_spec],
        residual_spec,
        residual_type,
        step=step,
    )(residual, foot, change)
    after1, back, final = owner(
        tables, got, after1, (norms1, after0), group=1, per=share, outs=everyone, outper=share, other="final"
    )
    rx1 = landed(spread(back))

    halves = divisor(share, (2, 1))
    half = share // halves
    chunks = []
    for c in range(halves):
        step = divisor(half, (2, 1))
        skip = c * half // step

        def at(spec, axis):
            shape, index = spec

            def moved(p, me, index=index, skip=skip, axis=axis):
                return tuple(skip + p if a == axis else 0 for a in range(index))

            return pl.BlockSpec(shape, moved)

        chunks.append(
            kernel(
                last_kernel, (half // step,),
                [
                    at(((step, voxels, every), 3), 0),
                    at(((step, groups, voxels, kb), 4), 0),
                    at(((step, every, kb), 3), 0),
                    at(((npix, ntm, step, own, kb), 5), 2),
                    at(((npix, ntm, step, own, kb), 5), 2),
                ],
                pl.BlockSpec((step, groups, voxels, kb), lambda p, *_: (p, 0, 0, 0)),
                array(half, groups, voxels, kb),
                prefetch=1, ntm=ntm, step=step,
            )(me, residual, foot, t1_old, rx0, rx1)
        )
    footprints_out = line_gather(chunks, "tm", ntm)

    gathered = lax.all_gather(final, "pix", axis=0)
    traces_out = kernel(
        flip_kernel, (blocks // several,),
        [pl.BlockSpec((npix, several, own, kb), lambda j: (0, j, 0, 0))],
        pl.BlockSpec((several, kb, frames), lambda j: (j, 0, 0)),
        array(blocks, kb, frames),
    )(gathered)
    return footprints_out, traces_out


def solution(mesh):
    npix, ntm = mesh.shape["pix"], mesh.shape["tm"]
    in_specs = (
        P("pix", None, "tm"),
        P("pix", None, None, None),
        P(None, None, "tm"),
        P("pix", None),
        P(),
    )
    out_specs = (P("pix", None, None, None), P(None, None, "tm"))

    def body(*args):
        return local(*args, npix=npix, ntm=ntm)

    return jax.shard_map(body, mesh=mesh, in_specs=in_specs, out_specs=out_specs, check_vma=False)
```

```python
import functools

import jax
import jax.numpy as jnp
from jax import lax
from jax.experimental import pallas as pl
from jax.experimental.pallas import tpu as pltpu
from jax.sharding import PartitionSpec as P


EPSILON = 1e-06
LIMIT = 24 * 2**20
SUBLANES = 8
f32 = jnp.float32
bf16 = jnp.bfloat16


def up8(n):
    return -(-n // SUBLANES) * SUBLANES


def divisor(n, limits):
    return max(m for m in limits if n % m == 0)


def split(x):
    high = x.astype(bf16)
    return high, (x - high.astype(f32)).astype(bf16)


def dot(a, b, ca, cb):
    return lax.dot_general(a, b, (((ca,), (cb,)), ((), ())), preferred_element_type=f32)


def rows_by_rows(a, b):
    left = jnp.concatenate(a, axis=1)
    right = jnp.concatenate([b[0], b[0]], axis=1)
    return dot(left, right, 1, 1) + dot(a[0], b[1], 1, 1)


def rows_by_columns(a, b, ca=1):
    n = b[0].shape[1]
    both = dot(a[0], jnp.concatenate(b, axis=1), ca, 0)
    return both[:, :n] + both[:, n:] + dot(a[1], b[0], ca, 0)


def full_spec(shape):
    return pl.BlockSpec(shape, lambda *_: (0,) * len(shape))


def whole(space):
    return pl.BlockSpec(memory_space=space)


def squares(x):
    return jnp.sum(x * x, axis=0, keepdims=True)


def first_kernel(bl, y, foot, *refs, parts, own, step, extra):
    t0s, t1s = refs[:step], refs[step:2 * step]
    base_out, pay = refs[2 * step:]
    at = pl.program_id(0) * step
    count = bl.shape[0]
    kb = foot.shape[3]
    for i in range(step):
        f0, f1 = split(foot[i, 0]), split(foot[i, 1])
        base = y[i].astype(f32) - rows_by_columns(f1, split(t1s[i][0]))
        base_out[i] = base
        residual = base - rows_by_columns(f0, split(t0s[i][0]))
        terms = rows_by_columns(split(residual), f0, 0)
        p = at + i
        pay[:, pl.ds(pl.multiple_of(p * own, SUBLANES), own), :] = terms.reshape(parts, own, kb)
        for g in range(2):
            norm = jnp.broadcast_to(squares(foot[i, g])[None], (parts, 1, kb))
            pay[:, pl.ds(count * own + g * count + p, 1), :] = norm

    @pl.when(at == 0)
    def _():
        shape = (extra, kb)
        where = lax.broadcasted_iota(jnp.int32, shape, 0) * kb + lax.broadcasted_iota(jnp.int32, shape, 1)
        listing = jnp.zeros(shape, jnp.int32)
        for p in range(count):
            for g in range(2):
                listing = jnp.where(where == 2 * p + g, bl[p, g], listing)
        pay[:, pay.shape[1] - extra:, :] = jnp.broadcast_to(listing.astype(f32)[None], (parts,) + shape)


def second_kernel(base, foot, rx, pay, *, parts, own, step):
    at = pl.program_id(0) * step
    kb = foot.shape[3]
    for i in range(step):
        f0, f1 = split(foot[i, 0]), split(foot[i, 1])
        trace = rx[:, i].reshape(parts * own, kb)
        residual = base[i] - rows_by_rows(f0, split(trace))
        terms = rows_by_columns(split(residual), f1, 0)
        pay[:, pl.ds(pl.multiple_of((at + i) * own, SUBLANES), own), :] = terms.reshape(parts, own, kb)


def prepare_kernel(order, pix, *refs, own, step):
    ins, out, flipped = refs[:step], refs[step], refs[step + 1]
    for i in range(step):
        flipped[i] = ins[i][0].T
        out[i] = flipped[i, pl.ds(pl.multiple_of(pix[0] * own, SUBLANES), own), :]


def owner_kernel(listing, place, order, rx, before, *refs, group, per, own, outs, outper, other):
    if other == "norms":
        after, back, norms1, totals, norms = refs
        norms1[...] = jnp.zeros(norms1.shape, f32)
        norms[...] = jnp.zeros(norms.shape, f32)
    elif other == "final":
        norms, after0, after, back, final, totals = refs
    else:
        norms, after, back, totals = refs
    sources = rx.shape[0]
    kb = rx.shape[2]
    bpg = before.shape[0]
    totals[...] = jnp.zeros(totals.shape, f32)

    @pl.loop(0, sources)
    def _(s):
        for i in range(per):
            p = s * per + i
            j = place[listing[p, group]] - group * bpg
            totals[j] = totals[j] + rx[s, i * own:(i + 1) * own, :]
            if other == "norms":
                row = per * own + i
                norms[j] = norms[j] + jnp.broadcast_to(rx[s, row:row + 1, :], (SUBLANES, kb))
                j1 = place[listing[p, 1]] - bpg
                row = per * own + per + i
                norms1[j1] = norms1[j1] + jnp.broadcast_to(rx[s, row:row + 1, :], (SUBLANES, kb))

    scale = kb * norms[:, 0:1, :] + EPSILON
    after[...] = jnp.maximum(before[...] + totals[...] / scale, 0.0)

    @pl.loop(0, outs)
    def _(s):
        for i in range(outper):
            j = place[listing[s * outper + i, group]] - group * bpg
            back[s, i * own:(i + 1) * own, :] = after[j]

    if other == "final":

        @pl.loop(0, bpg, unroll=4)
        def _(j):
            final[order[j]] = after0[j]
            final[order[bpg + j]] = after[j]


def owner(tables, rx, before, extra, *, group, per, outs, outper, other):
    bpg, own, kb = before.shape
    norms_shape = (bpg, SUBLANES, kb)
    shapes = [before.shape, (outs, outper * own, kb)]
    if other == "norms":
        shapes.append(norms_shape)
    if other == "final":
        shapes.append((2 * bpg, own, kb))
    scratch = [pltpu.VMEM(before.shape, f32)]
    if other == "norms":
        scratch.append(pltpu.VMEM(norms_shape, f32))
    return pl.pallas_call(
        functools.partial(owner_kernel, group=group, per=per, own=own, outs=outs, outper=outper, other=other),
        in_specs=[whole(pltpu.SMEM)] * 3 + [whole(pltpu.VMEM)] * (2 + len(extra)),
        out_specs=[whole(pltpu.VMEM)] * len(shapes),
        scratch_shapes=scratch,
        out_shape=[jax.ShapeDtypeStruct(shape, f32) for shape in shapes],
        compiler_params=pltpu.CompilerParams(vmem_limit_bytes=LIMIT),
        name="owner",
    )(*tables, rx, before, *extra)


def incoming(rx, i, me, ntm):
    pieces = []
    for s in range(ntm):
        piece = rx[:, lax.rem(me + (ntm - s), ntm), i]
        pieces.append(piece.reshape(piece.shape[0] * piece.shape[1], piece.shape[2]))
    return jnp.concatenate(pieces, axis=0)


def outgoing(pay, terms, p, me, ntm):
    npix, kb = pay.shape[0], terms.shape[1]
    own = terms.shape[0] // (npix * ntm)
    for s in range(ntm):
        piece = terms[s * npix * own:(s + 1) * npix * own].reshape(npix, own, kb)
        to = lax.rem(me + (ntm - s), ntm)
        pay[:, to, p * own:(p + 1) * own, :] = piece


def footprint_phase(residual, f0, f1, t0, t1):
    kb = f0.shape[1]
    scale0 = kb * squares(t0) + EPSILON
    scale1 = kb * squares(t1) + EPSILON
    s0, s1 = split(t0), split(t1)
    n0 = jnp.maximum(f0 + rows_by_columns(split(residual), s0) / scale0, 0.0)
    residual = residual - rows_by_rows(split(n0 - f0), s0)
    n1 = jnp.maximum(f1 + rows_by_columns(split(residual), s1) / scale1, 0.0)
    return residual, n0, n1, s1


def third_kernel(*refs, ntm):
    ys, t0s = refs[:ntm], refs[ntm:2 * ntm]
    rx1, foot, residual_out, foot_out, t0_out, t1_out, pay = refs[2 * ntm:]
    me = lax.axis_index("tm")
    count, kb = foot.shape[0], foot.shape[3]
    own = (pay.shape[2] - up8(2 * count)) // count
    for i in range(count):
        f0, f1 = foot[i, 0], foot[i, 1]
        y = jnp.concatenate([ref[i] for ref in ys], axis=1)
        t0 = jnp.concatenate([ref[:, i].reshape(ref.shape[0] * ref.shape[2], kb) for ref in t0s], axis=0)
        t1 = incoming(rx1, i, me, ntm)
        residual = y - rows_by_rows(split(f0), split(t0)) - rows_by_rows(split(f1), split(t1))
        residual, n0, n1, s1 = footprint_phase(residual, f0, f1, t0, t1)
        residual = residual - rows_by_rows(split(n1 - f1), s1)
        residual_out[i] = residual
        foot_out[i, 0] = n0
        foot_out[i, 1] = n1
        t0_out[i] = t0
        t1_out[i] = t1
        outgoing(pay, rows_by_columns(split(residual), split(n0), 0), i, me, ntm)
        for g, new in enumerate((n0, n1)):
            norm = jnp.broadcast_to(squares(new)[None, None], pay.shape[:2] + (1, kb))
            row = count * own + g * count + i
            pay[:, :, row:row + 1, :] = norm


def fourth_kernel(residual_in, foot, told, rx, residual_out, pay, *, ntm):
    me = lax.axis_index("tm")
    for i in range(told.shape[0]):
        change = incoming(rx, i, me, ntm) - told[i]
        residual = residual_in[i] - rows_by_rows(split(foot[i, 0]), split(change))
        residual_out[i] = residual
        outgoing(pay, rows_by_columns(split(residual), split(foot[i, 1]), 0), i, me, ntm)


def last_kernel(residual_in, foot, told, rx0, rx1, foot_out, *, ntm, skip):
    me = lax.axis_index("tm")
    for o in range(foot_out.shape[0]):
        i = skip + o
        f0, f1 = foot[i, 0], foot[i, 1]
        t0 = incoming(rx0, i, me, ntm)
        t1 = incoming(rx1, i, me, ntm)
        residual = residual_in[i] - rows_by_rows(split(f1), split(t1 - told[i]))
        _, n0, n1, _ = footprint_phase(residual, f0, f1, t0, t1)
        foot_out[o, 0] = n0
        foot_out[o, 1] = n1


def flip_kernel(rx, out):
    npix, count, own, kb = rx.shape
    for j in range(count):
        out[j] = rx[:, j].reshape(npix * own, kb).T


def early_kernel(*refs, n, count, axis):
    chunks, rest, out, sems = refs[:count], refs[count:-2], refs[-2], refs[-1]
    me = lax.axis_index(axis)
    per = chunks[0].shape[0]
    from_left, from_right = rest[:(n - 2) * count], rest[(n - 2) * count:]

    def copy(source, s, c):
        place = lax.rem(me + s, n) * (count * per) + c * per
        return pltpu.make_async_copy(source, out.at[pl.ds(place, per)], sems.at[s, c])

    def every(act):
        for c in range(count):
            act(copy(chunks[c], 0, c))
            for s in range(1, n):
                if s <= n - 2:

                    @pl.when(me + s < n)
                    def _():
                        act(copy(from_right[(s - 1) * count + c], s, c))

                if s >= 2:

                    @pl.when(me + s >= n)
                    def _():
                        act(copy(from_left[(n - s - 1) * count + c], s, c))

    every(lambda one: one.start())
    every(lambda one: one.wait())


def ends_kernel(before, *refs, n, count, axis):
    from_left, from_right, out, sems = refs[:count], refs[count:2 * count], refs[-2], refs[-1]
    me = lax.axis_index(axis)
    per = from_left[0].shape[0]

    def move(sources, place):
        for c in range(count):
            pltpu.make_async_copy(
                sources[c], out.at[pl.ds((place * count + c) * per, per)], sems.at[c]
            ).start()
        for c in range(count):
            pltpu.make_async_copy(
                sources[c], out.at[pl.ds((place * count + c) * per, per)], sems.at[c]
            ).wait()

    @pl.when(me == 0)
    def _():
        move(from_right, n - 1)

    @pl.when(me == n - 1)
    def _():
        move(from_left, 0)


def line_gather(chunks, axis, n):
    size = sum(x.shape[0] for x in chunks)
    rest = chunks[0].shape[1:]
    left, right = list(chunks), list(chunks)
    from_left, from_right = {}, {}
    for s in range(1, n):
        for c in range(len(chunks)):
            left[c] = lax.ppermute(left[c], axis, [(j, j + 1) for j in range(n - 1)])
            right[c] = lax.ppermute(right[c], axis, [(j, j - 1) for j in range(1, n)])
            from_left[s, c], from_right[s, c] = left[c], right[c]
    shape = jax.ShapeDtypeStruct((n * size,) + rest, f32)
    early = [s for s in range(1, n - 1)]
    sources = list(chunks) + [d[s, c] for d in (from_left, from_right) for s in early for c in range(len(chunks))]
    out = pl.pallas_call(
        functools.partial(early_kernel, n=n, count=len(chunks), axis=axis),
        in_specs=[whole(pltpu.VMEM)] * len(sources),
        out_specs=whole(pltpu.HBM),
        out_shape=shape,
        scratch_shapes=[pltpu.SemaphoreType.DMA((n, len(chunks)))],
        compiler_params=pltpu.CompilerParams(vmem_limit_bytes=LIMIT),
        name="early",
    )(*sources)
    ends = [d[n - 1, c] for d in (from_left, from_right) for c in range(len(chunks))]
    return pl.pallas_call(
        functools.partial(ends_kernel, n=n, count=len(chunks), axis=axis),
        in_specs=[whole(pltpu.HBM)] + [whole(pltpu.VMEM)] * len(ends),
        out_specs=whole(pltpu.HBM),
        out_shape=shape,
        input_output_aliases={0: 0},
        scratch_shapes=[pltpu.SemaphoreType.DMA((len(chunks),))],
        compiler_params=pltpu.CompilerParams(vmem_limit_bytes=LIMIT),
        name="ends",
    )(out, *ends)


def local(recording, footprints, traces, block_list, block_order, *, npix, ntm):
    count, voxels, frames = recording.shape
    groups, kb = footprints.shape[1], footprints.shape[3]
    blocks = traces.shape[0]
    bpg = blocks // groups
    own = frames // npix
    share = count // ntm
    everyone = npix * ntm
    every = frames * ntm
    pix, tm = lax.axis_index("pix"), lax.axis_index("tm")
    me = jnp.reshape(tm, (1,)).astype(jnp.int32)

    def kernel(body, grid, in_specs, out_specs, out_shape, prefetch=0, scratch=(), limit=None, **static):
        return pl.pallas_call(
            functools.partial(body, **static),
            grid_spec=pltpu.PrefetchScalarGridSpec(
                num_scalar_prefetch=prefetch,
                grid=grid,
                in_specs=in_specs,
                out_specs=out_specs,
                scratch_shapes=scratch,
            ),
            out_shape=out_shape,
            compiler_params=pltpu.CompilerParams(vmem_limit_bytes=limit),
        )

    def resident(body, out_shape, **static):
        def run(*operands):
            return pl.pallas_call(
                functools.partial(body, **static),
                in_specs=[whole(pltpu.VMEM)] * len(operands),
                out_specs=jax.tree.map(lambda _: whole(pltpu.VMEM), out_shape),
                out_shape=out_shape,
                compiler_params=pltpu.CompilerParams(vmem_limit_bytes=LIMIT),
            )(*operands)

        return run

    def array(*shape):
        return jax.ShapeDtypeStruct(shape, f32)

    def exchange(x, axes):
        return lax.all_to_all(x, axes, 0, 0, tiled=True)

    y_pieces = []
    for s in range(ntm):
        to = lax.rem(tm + s, ntm)
        piece = lax.dynamic_slice_in_dim(recording, to * share, share, 0).astype(f32)
        y_pieces.append(lax.ppermute(piece, "tm", [(j, (j + s) % ntm) for j in range(ntm)]) if s else piece)

    pos_rows = up8(-(-count * groups // kb))
    place = jnp.zeros((blocks,), jnp.int32).at[block_order].set(jnp.arange(blocks, dtype=jnp.int32))

    step = divisor(count, (4, 2, 1))
    rows = count * own + up8(groups * count)
    foot_spec = pl.BlockSpec((step, groups, voxels, kb), lambda p, *_: (p, 0, 0, 0))
    patch_spec = pl.BlockSpec((step, voxels, frames), lambda p, *_: (p, 0, 0))

    def block_spec(i, g):
        return pl.BlockSpec((1, kb, frames), lambda p, bl: (bl[p * step + i, g], 0, 0))

    base, pay = kernel(
        first_kernel, (count // step,),
        [patch_spec, foot_spec] + [block_spec(i, g) for g in range(groups) for i in range(step)],
        [patch_spec, full_spec((npix, rows + pos_rows, kb))],
        [array(count, voxels, frames), array(npix, rows + pos_rows, kb)],
        prefetch=1, parts=npix, own=own, step=step, extra=pos_rows,
    )(block_list, recording, footprints, *[traces] * (groups * step))
    got = exchange(pay, "pix")

    several = divisor(bpg, (8, 4, 2, 1))
    whereabouts = jnp.reshape(pix, (1,)).astype(jnp.int32)

    def prepared(g):
        def ordered_spec(i):
            return pl.BlockSpec(
                (1, kb, frames), lambda b, order, pix: (order[g * bpg + b * several + i], 0, 0)
            )

        return kernel(
            prepare_kernel, (bpg // several,),
            [ordered_spec(i) for i in range(several)],
            pl.BlockSpec((several, own, kb), lambda b, *_: (b, 0, 0)),
            array(bpg, own, kb),
            prefetch=2, scratch=[pltpu.VMEM((several, frames, kb), f32)], own=own, step=several,
        )(block_order, whereabouts, *[traces] * several)

    before0, before1 = prepared(0), prepared(1)
    own_foot = lax.dynamic_slice_in_dim(footprints, tm * share, share, 0)

    listing = got[:, rows:, :].reshape(npix, -1)[:, :count * groups].reshape(npix * count, groups)
    tables = (listing.astype(jnp.int32), place, block_order)
    after0, back, norms1 = owner(
        tables, got, before0, (), group=0, per=count, outs=npix, outper=count, other="norms"
    )
    rx0 = exchange(back, "pix").reshape(npix, count, own, kb)

    t0_pieces = []
    for s in range(ntm):
        to = lax.rem(tm + s, ntm)
        piece = lax.dynamic_slice_in_dim(rx0, to * share, share, 1)
        t0_pieces.append(lax.ppermute(piece, "tm", [(j, (j + s) % ntm) for j in range(ntm)]) if s else piece)

    pay = kernel(
        second_kernel, (count // step,),
        [patch_spec, foot_spec, pl.BlockSpec((npix, step, own, kb), lambda p: (0, p, 0, 0))],
        full_spec((npix, count * own, kb)),
        array(npix, count * own, kb),
        parts=npix, own=own, step=step,
    )(base, footprints, rx0)
    after1, back = owner(
        tables, exchange(pay, "pix"), before1, (norms1,),
        group=1, per=count, outs=everyone, outper=share, other=None,
    )

    def spread(x):
        return exchange(x.reshape(everyone, x.shape[-2], kb), ("pix", "tm"))

    def landed(x):
        return x.reshape(npix, ntm, share, own, kb)

    rx1 = landed(spread(back))

    residual_type, trace_type = array(share, voxels, every), array(share, every, kb)
    wide = (npix, ntm, share * own + up8(groups * share), kb)
    narrow = (npix, ntm, share * own, kb)
    residual, foot, t0_old, t1_old, pay = resident(
        third_kernel, [residual_type, array(share, groups, voxels, kb), trace_type, trace_type, array(*wide)], ntm=ntm
    )(*y_pieces, *t0_pieces, rx1, own_foot)

    got = spread(pay)
    after0, back, norms1 = owner(
        tables, got, after0, (), group=0, per=share, outs=everyone, outper=share, other="norms"
    )
    rx0 = landed(spread(back))
    residual, pay = resident(fourth_kernel, [residual_type, array(*narrow)], ntm=ntm)(residual, foot, t0_old, rx0)
    got = spread(pay)
    after1, back, final = owner(
        tables, got, after1, (norms1, after0), group=1, per=share, outs=everyone, outper=share, other="final"
    )
    rx1 = landed(spread(back))

    halves = divisor(share, (2, 1))
    half = share // halves
    chunks = [
        resident(last_kernel, array(half, groups, voxels, kb), ntm=ntm, skip=c * half)(residual, foot, t1_old, rx0, rx1)
        for c in range(halves)
    ]
    footprints_out = line_gather(chunks, "tm", ntm)

    gathered = lax.all_gather(final, "pix", axis=0)
    traces_out = kernel(
        flip_kernel, (blocks // several,),
        [pl.BlockSpec((npix, several, own, kb), lambda j: (0, j, 0, 0))],
        pl.BlockSpec((several, kb, frames), lambda j: (j, 0, 0)),
        array(blocks, kb, frames),
        limit=LIMIT,
    )(gathered)
    return footprints_out, traces_out


def solution(mesh):
    npix, ntm = mesh.shape["pix"], mesh.shape["tm"]
    in_specs = (
        P("pix", None, "tm"),
        P("pix", None, None, None),
        P(None, None, "tm"),
        P("pix", None),
        P(),
    )
    out_specs = (P("pix", None, None, None), P(None, None, "tm"))

    def body(*args):
        return local(*args, npix=npix, ntm=ntm)

    return jax.shard_map(body, mesh=mesh, in_specs=in_specs, out_specs=out_specs, check_vma=False)
```

```python
import functools

import jax
import jax.numpy as jnp
from jax import lax
from jax.experimental import pallas as pl
from jax.experimental.pallas import tpu as pltpu
from jax.sharding import PartitionSpec as P


EPSILON = 1e-06
LIMIT = 24 * 2**20
SUBLANES = 8
f32 = jnp.float32
bf16 = jnp.bfloat16


def up8(n):
    return -(-n // SUBLANES) * SUBLANES


def divisor(n, limits):
    return max(m for m in limits if n % m == 0)


def split(x):
    high = x.astype(bf16)
    return high, (x - high.astype(f32)).astype(bf16)


def dot(a, b, ca, cb):
    return lax.dot_general(a, b, (((ca,), (cb,)), ((), ())), preferred_element_type=f32)


def rows_by_rows(a, b):
    left = jnp.concatenate(a, axis=1)
    right = jnp.concatenate([b[0], b[0]], axis=1)
    return dot(left, right, 1, 1) + dot(a[0], b[1], 1, 1)


def rows_by_columns(a, b, ca=1):
    n = b[0].shape[1]
    both = dot(a[0], jnp.concatenate(b, axis=1), ca, 0)
    return both[:, :n] + both[:, n:] + dot(a[1], b[0], ca, 0)


def full_spec(shape):
    return pl.BlockSpec(shape, lambda *_: (0,) * len(shape))


def whole(space):
    return pl.BlockSpec(memory_space=space)


def squares(x):
    return jnp.sum(x * x, axis=0, keepdims=True)


def first_kernel(bl, y, foot, *refs, parts, own, step, extra):
    t0s, t1s = refs[:step], refs[step:2 * step]
    base_out, pay = refs[2 * step:]
    at = pl.program_id(0) * step
    count = bl.shape[0]
    kb = foot.shape[3]
    for i in range(step):
        f0, f1 = split(foot[i, 0]), split(foot[i, 1])
        base = y[i].astype(f32) - rows_by_columns(f1, split(t1s[i][0]))
        base_out[i] = base
        residual = base - rows_by_columns(f0, split(t0s[i][0]))
        terms = rows_by_columns(split(residual), f0, 0)
        p = at + i
        pay[:, pl.ds(pl.multiple_of(p * own, SUBLANES), own), :] = terms.reshape(parts, own, kb)
        for g in range(2):
            norm = jnp.broadcast_to(squares(foot[i, g])[None], (parts, 1, kb))
            pay[:, pl.ds(count * own + g * count + p, 1), :] = norm

    @pl.when(at == 0)
    def _():
        shape = (extra, kb)
        where = lax.broadcasted_iota(jnp.int32, shape, 0) * kb + lax.broadcasted_iota(jnp.int32, shape, 1)
        listing = jnp.zeros(shape, jnp.int32)
        for p in range(count):
            for g in range(2):
                listing = jnp.where(where == 2 * p + g, bl[p, g], listing)
        pay[:, pay.shape[1] - extra:, :] = jnp.broadcast_to(listing.astype(f32)[None], (parts,) + shape)


def second_kernel(base, foot, rx, pay, *, parts, own, step):
    at = pl.program_id(0) * step
    kb = foot.shape[3]
    for i in range(step):
        f0, f1 = split(foot[i, 0]), split(foot[i, 1])
        trace = rx[:, i].reshape(parts * own, kb)
        residual = base[i] - rows_by_rows(f0, split(trace))
        terms = rows_by_columns(split(residual), f1, 0)
        pay[:, pl.ds(pl.multiple_of((at + i) * own, SUBLANES), own), :] = terms.reshape(parts, own, kb)


def prepare_kernel(order, pix, *refs, own, step):
    ins, out, flipped = refs[:step], refs[step], refs[step + 1]
    for i in range(step):
        flipped[i] = ins[i][0].T
        out[i] = flipped[i, pl.ds(pl.multiple_of(pix[0] * own, SUBLANES), own), :]


def owner_kernel(listing, place, order, rx, before, *refs, group, per, own, outs, outper, other):
    if other == "norms":
        after, back, norms1, totals, norms = refs
        norms1[...] = jnp.zeros(norms1.shape, f32)
        norms[...] = jnp.zeros(norms.shape, f32)
    elif other == "final":
        norms, after0, after, back, final, totals = refs
    else:
        norms, after, back, totals = refs
    sources = rx.shape[0]
    kb = rx.shape[2]
    bpg = before.shape[0]
    totals[...] = jnp.zeros(totals.shape, f32)

    @pl.loop(0, sources)
    def _(s):
        for i in range(per):
            p = s * per + i
            j = place[listing[p, group]] - group * bpg
            totals[j] = totals[j] + rx[s, i * own:(i + 1) * own, :]
            if other == "norms":
                row = per * own + i
                norms[j] = norms[j] + jnp.broadcast_to(rx[s, row:row + 1, :], (SUBLANES, kb))
                j1 = place[listing[p, 1]] - bpg
                row = per * own + per + i
                norms1[j1] = norms1[j1] + jnp.broadcast_to(rx[s, row:row + 1, :], (SUBLANES, kb))

    scale = kb * norms[:, 0:1, :] + EPSILON
    after[...] = jnp.maximum(before[...] + totals[...] / scale, 0.0)

    @pl.loop(0, outs)
    def _(s):
        for i in range(outper):
            j = place[listing[s * outper + i, group]] - group * bpg
            back[s, i * own:(i + 1) * own, :] = after[j]

    if other == "final":

        @pl.loop(0, bpg, unroll=4)
        def _(j):
            final[order[j]] = after0[j]
            final[order[bpg + j]] = after[j]


def owner(tables, rx, before, extra, *, group, per, outs, outper, other):
    bpg, own, kb = before.shape
    norms_shape = (bpg, SUBLANES, kb)
    shapes = [before.shape, (outs, outper * own, kb)]
    if other == "norms":
        shapes.append(norms_shape)
    if other == "final":
        shapes.append((2 * bpg, own, kb))
    scratch = [pltpu.VMEM(before.shape, f32)]
    if other == "norms":
        scratch.append(pltpu.VMEM(norms_shape, f32))
    return pl.pallas_call(
        functools.partial(owner_kernel, group=group, per=per, own=own, outs=outs, outper=outper, other=other),
        in_specs=[whole(pltpu.SMEM)] * 3 + [whole(pltpu.VMEM)] * (2 + len(extra)),
        out_specs=[whole(pltpu.VMEM)] * len(shapes),
        scratch_shapes=scratch,
        out_shape=[jax.ShapeDtypeStruct(shape, f32) for shape in shapes],
        compiler_params=pltpu.CompilerParams(vmem_limit_bytes=LIMIT),
        name="owner",
    )(*tables, rx, before, *extra)


def incoming(rx, i, me, ntm):
    pieces = []
    for s in range(ntm):
        piece = rx[:, lax.rem(me + (ntm - s), ntm), i]
        pieces.append(piece.reshape(piece.shape[0] * piece.shape[1], piece.shape[2]))
    return jnp.concatenate(pieces, axis=0)


def outgoing(pay, terms, p, me, ntm):
    npix, kb = pay.shape[0], terms.shape[1]
    own = terms.shape[0] // (npix * ntm)
    for s in range(ntm):
        piece = terms[s * npix * own:(s + 1) * npix * own].reshape(npix, own, kb)
        to = lax.rem(me + (ntm - s), ntm)
        pay[:, to, p * own:(p + 1) * own, :] = piece


def footprint_phase(residual, f0, f1, t0, t1):
    kb = f0.shape[1]
    scale0 = kb * squares(t0) + EPSILON
    scale1 = kb * squares(t1) + EPSILON
    s0, s1 = split(t0), split(t1)
    n0 = jnp.maximum(f0 + rows_by_columns(split(residual), s0) / scale0, 0.0)
    residual = residual - rows_by_rows(split(n0 - f0), s0)
    n1 = jnp.maximum(f1 + rows_by_columns(split(residual), s1) / scale1, 0.0)
    return residual, n0, n1, s1


def third_kernel(*refs, ntm):
    ys, t0s = refs[:ntm], refs[ntm:2 * ntm]
    rx1, foot, residual_out, foot_out, t0_out, t1_out, pay = refs[2 * ntm:]
    me = lax.axis_index("tm")
    count, kb = foot.shape[0], foot.shape[3]
    own = (pay.shape[2] - up8(2 * count)) // count
    for i in range(count):
        f0, f1 = foot[i, 0], foot[i, 1]
        y = jnp.concatenate([ref[i] for ref in ys], axis=1)
        t0 = jnp.concatenate([ref[:, i].reshape(ref.shape[0] * ref.shape[2], kb) for ref in t0s], axis=0)
        t1 = incoming(rx1, i, me, ntm)
        residual = y - rows_by_rows(split(f0), split(t0)) - rows_by_rows(split(f1), split(t1))
        residual, n0, n1, s1 = footprint_phase(residual, f0, f1, t0, t1)
        residual = residual - rows_by_rows(split(n1 - f1), s1)
        residual_out[i] = residual
        foot_out[i, 0] = n0
        foot_out[i, 1] = n1
        t0_out[i] = t0
        t1_out[i] = t1
        outgoing(pay, rows_by_columns(split(residual), split(n0), 0), i, me, ntm)
        for g, new in enumerate((n0, n1)):
            norm = jnp.broadcast_to(squares(new)[None, None], pay.shape[:2] + (1, kb))
            row = count * own + g * count + i
            pay[:, :, row:row + 1, :] = norm


def fourth_kernel(residual_in, foot, told, rx, residual_out, pay, *, ntm):
    me = lax.axis_index("tm")
    for i in range(told.shape[0]):
        change = incoming(rx, i, me, ntm) - told[i]
        residual = residual_in[i] - rows_by_rows(split(foot[i, 0]), split(change))
        residual_out[i] = residual
        outgoing(pay, rows_by_columns(split(residual), split(foot[i, 1]), 0), i, me, ntm)


def last_kernel(residual_in, foot, told, rx0, rx1, foot_out, *, ntm, skip):
    me = lax.axis_index("tm")
    for o in range(foot_out.shape[0]):
        i = skip + o
        f0, f1 = foot[i, 0], foot[i, 1]
        t0 = incoming(rx0, i, me, ntm)
        t1 = incoming(rx1, i, me, ntm)
        residual = residual_in[i] - rows_by_rows(split(f1), split(t1 - told[i]))
        _, n0, n1, _ = footprint_phase(residual, f0, f1, t0, t1)
        foot_out[o, 0] = n0
        foot_out[o, 1] = n1


def flip_kernel(*refs, origins):
    pieces, out, frames = refs[:-2], refs[-2], refs[-1]
    count, own, _ = pieces[0].shape
    places = [pl.multiple_of(o * own, SUBLANES) for o in origins(lax.axis_index("pix"))]
    for j in range(count):
        for piece, place in zip(pieces, places):
            frames[j, pl.ds(place, own), :] = piece[j]
        out[j] = frames[j].T


def pair_gather(x, axis, n):
    chips = n // 2
    power = chips & (chips - 1) == 0

    def source(chip, s):
        return chip ^ s if power else lax.rem(chip + s, chips)

    def target(chip, s):
        return chip ^ s if power else (chip - s) % chips

    pieces = []
    for s in range(chips):
        perm = [(j, target(j // 2, s) * 2 + j % 2) for j in range(n)]
        pieces.append(lax.ppermute(x, axis, perm) if s else x)
    swap = [(j, j ^ 1) for j in range(n)]
    for s in range(chips):
        pieces.append(lax.ppermute(pieces[s], axis, swap))

    def origins(me):
        chip, core = me // 2, lax.rem(me, 2)
        return [source(chip, s) * 2 + c for c in (core, 1 - core) for s in range(chips)]

    return pieces, origins


def early_kernel(*refs, n, count, axis):
    chunks, rest, out, sems = refs[:count], refs[count:-2], refs[-2], refs[-1]
    me = lax.axis_index(axis)
    per = chunks[0].shape[0]
    from_left, from_right = rest[:(n - 2) * count], rest[(n - 2) * count:]

    def copy(source, s, c):
        place = lax.rem(me + s, n) * (count * per) + c * per
        return pltpu.make_async_copy(source, out.at[pl.ds(place, per)], sems.at[s, c])

    def every(act):
        for c in range(count):
            act(copy(chunks[c], 0, c))
            for s in range(1, n):
                if s <= n - 2:

                    @pl.when(me + s < n)
                    def _():
                        act(copy(from_right[(s - 1) * count + c], s, c))

                if s >= 2:

                    @pl.when(me + s >= n)
                    def _():
                        act(copy(from_left[(n - s - 1) * count + c], s, c))

    every(lambda one: one.start())
    every(lambda one: one.wait())


def ends_kernel(before, *refs, n, count, axis):
    from_left, from_right, out, sems = refs[:count], refs[count:2 * count], refs[-2], refs[-1]
    me = lax.axis_index(axis)
    per = from_left[0].shape[0]

    def move(sources, place):
        for c in range(count):
            pltpu.make_async_copy(
                sources[c], out.at[pl.ds((place * count + c) * per, per)], sems.at[c]
            ).start()
        for c in range(count):
            pltpu.make_async_copy(
                sources[c], out.at[pl.ds((place * count + c) * per, per)], sems.at[c]
            ).wait()

    @pl.when(me == 0)
    def _():
        move(from_right, n - 1)

    @pl.when(me == n - 1)
    def _():
        move(from_left, 0)


def line_gather(chunks, axis, n):
    size = sum(x.shape[0] for x in chunks)
    rest = chunks[0].shape[1:]
    left, right = list(chunks), list(chunks)
    from_left, from_right = {}, {}
    for s in range(1, n):
        for c in range(len(chunks)):
            left[c] = lax.ppermute(left[c], axis, [(j, j + 1) for j in range(n - 1)])
            right[c] = lax.ppermute(right[c], axis, [(j, j - 1) for j in range(1, n)])
            from_left[s, c], from_right[s, c] = left[c], right[c]
    shape = jax.ShapeDtypeStruct((n * size,) + rest, f32)
    early = [s for s in range(1, n - 1)]
    sources = list(chunks) + [d[s, c] for d in (from_left, from_right) for s in early for c in range(len(chunks))]
    out = pl.pallas_call(
        functools.partial(early_kernel, n=n, count=len(chunks), axis=axis),
        in_specs=[whole(pltpu.VMEM)] * len(sources),
        out_specs=whole(pltpu.HBM),
        out_shape=shape,
        scratch_shapes=[pltpu.SemaphoreType.DMA((n, len(chunks)))],
        compiler_params=pltpu.CompilerParams(vmem_limit_bytes=LIMIT),
        name="early",
    )(*sources)
    ends = [d[n - 1, c] for d in (from_left, from_right) for c in range(len(chunks))]
    return pl.pallas_call(
        functools.partial(ends_kernel, n=n, count=len(chunks), axis=axis),
        in_specs=[whole(pltpu.HBM)] + [whole(pltpu.VMEM)] * len(ends),
        out_specs=whole(pltpu.HBM),
        out_shape=shape,
        input_output_aliases={0: 0},
        scratch_shapes=[pltpu.SemaphoreType.DMA((len(chunks),))],
        compiler_params=pltpu.CompilerParams(vmem_limit_bytes=LIMIT),
        name="ends",
    )(out, *ends)


def local(recording, footprints, traces, block_list, block_order, *, npix, ntm):
    count, voxels, frames = recording.shape
    groups, kb = footprints.shape[1], footprints.shape[3]
    blocks = traces.shape[0]
    bpg = blocks // groups
    own = frames // npix
    share = count // ntm
    everyone = npix * ntm
    every = frames * ntm
    pix, tm = lax.axis_index("pix"), lax.axis_index("tm")
    me = jnp.reshape(tm, (1,)).astype(jnp.int32)

    def kernel(body, grid, in_specs, out_specs, out_shape, prefetch=0, scratch=(), limit=None, **static):
        return pl.pallas_call(
            functools.partial(body, **static),
            grid_spec=pltpu.PrefetchScalarGridSpec(
                num_scalar_prefetch=prefetch,
                grid=grid,
                in_specs=in_specs,
                out_specs=out_specs,
                scratch_shapes=scratch,
            ),
            out_shape=out_shape,
            compiler_params=pltpu.CompilerParams(vmem_limit_bytes=limit),
        )

    def resident(body, out_shape, **static):
        def run(*operands):
            return pl.pallas_call(
                functools.partial(body, **static),
                in_specs=[whole(pltpu.VMEM)] * len(operands),
                out_specs=jax.tree.map(lambda _: whole(pltpu.VMEM), out_shape),
                out_shape=out_shape,
                compiler_params=pltpu.CompilerParams(vmem_limit_bytes=LIMIT),
            )(*operands)

        return run

    def array(*shape):
        return jax.ShapeDtypeStruct(shape, f32)

    def exchange(x, axes):
        return lax.all_to_all(x, axes, 0, 0, tiled=True)

    y_pieces = []
    for s in range(ntm):
        to = lax.rem(tm + s, ntm)
        piece = lax.dynamic_slice_in_dim(recording, to * share, share, 0).astype(f32)
        y_pieces.append(lax.ppermute(piece, "tm", [(j, (j + s) % ntm) for j in range(ntm)]) if s else piece)

    pos_rows = up8(-(-count * groups // kb))
    place = jnp.zeros((blocks,), jnp.int32).at[block_order].set(jnp.arange(blocks, dtype=jnp.int32))

    step = divisor(count, (4, 2, 1))
    rows = count * own + up8(groups * count)
    foot_spec = pl.BlockSpec((step, groups, voxels, kb), lambda p, *_: (p, 0, 0, 0))
    patch_spec = pl.BlockSpec((step, voxels, frames), lambda p, *_: (p, 0, 0))

    def block_spec(i, g):
        return pl.BlockSpec((1, kb, frames), lambda p, bl: (bl[p * step + i, g], 0, 0))

    base, pay = kernel(
        first_kernel, (count // step,),
        [patch_spec, foot_spec] + [block_spec(i, g) for g in range(groups) for i in range(step)],
        [patch_spec, full_spec((npix, rows + pos_rows, kb))],
        [array(count, voxels, frames), array(npix, rows + pos_rows, kb)],
        prefetch=1, parts=npix, own=own, step=step, extra=pos_rows,
    )(block_list, recording, footprints, *[traces] * (groups * step))
    got = exchange(pay, "pix")

    several = divisor(bpg, (8, 4, 2, 1))
    whereabouts = jnp.reshape(pix, (1,)).astype(jnp.int32)

    def prepared(g):
        def ordered_spec(i):
            return pl.BlockSpec(
                (1, kb, frames), lambda b, order, pix: (order[g * bpg + b * several + i], 0, 0)
            )

        return kernel(
            prepare_kernel, (bpg // several,),
            [ordered_spec(i) for i in range(several)],
            pl.BlockSpec((several, own, kb), lambda b, *_: (b, 0, 0)),
            array(bpg, own, kb),
            prefetch=2, scratch=[pltpu.VMEM((several, frames, kb), f32)], own=own, step=several,
        )(block_order, whereabouts, *[traces] * several)

    before0, before1 = prepared(0), prepared(1)
    own_foot = lax.dynamic_slice_in_dim(footprints, tm * share, share, 0)

    listing = got[:, rows:, :].reshape(npix, -1)[:, :count * groups].reshape(npix * count, groups)
    tables = (listing.astype(jnp.int32), place, block_order)
    after0, back, norms1 = owner(
        tables, got, before0, (), group=0, per=count, outs=npix, outper=count, other="norms"
    )
    rx0 = exchange(back, "pix").reshape(npix, count, own, kb)

    t0_pieces = []
    for s in range(ntm):
        to = lax.rem(tm + s, ntm)
        piece = lax.dynamic_slice_in_dim(rx0, to * share, share, 1)
        t0_pieces.append(lax.ppermute(piece, "tm", [(j, (j + s) % ntm) for j in range(ntm)]) if s else piece)

    pay = kernel(
        second_kernel, (count // step,),
        [patch_spec, foot_spec, pl.BlockSpec((npix, step, own, kb), lambda p: (0, p, 0, 0))],
        full_spec((npix, count * own, kb)),
        array(npix, count * own, kb),
        parts=npix, own=own, step=step,
    )(base, footprints, rx0)
    after1, back = owner(
        tables, exchange(pay, "pix"), before1, (norms1,),
        group=1, per=count, outs=everyone, outper=share, other=None,
    )

    def spread(x):
        return exchange(x.reshape(everyone, x.shape[-2], kb), ("pix", "tm"))

    def landed(x):
        return x.reshape(npix, ntm, share, own, kb)

    rx1 = landed(spread(back))

    residual_type, trace_type = array(share, voxels, every), array(share, every, kb)
    wide = (npix, ntm, share * own + up8(groups * share), kb)
    narrow = (npix, ntm, share * own, kb)
    residual, foot, t0_old, t1_old, pay = resident(
        third_kernel, [residual_type, array(share, groups, voxels, kb), trace_type, trace_type, array(*wide)], ntm=ntm
    )(*y_pieces, *t0_pieces, rx1, own_foot)

    got = spread(pay)
    after0, back, norms1 = owner(
        tables, got, after0, (), group=0, per=share, outs=everyone, outper=share, other="norms"
    )
    rx0 = landed(spread(back))
    residual, pay = resident(fourth_kernel, [residual_type, array(*narrow)], ntm=ntm)(residual, foot, t0_old, rx0)
    got = spread(pay)
    after1, back, final = owner(
        tables, got, after1, (norms1, after0), group=1, per=share, outs=everyone, outper=share, other="final"
    )
    rx1 = landed(spread(back))

    halves = divisor(share, (2, 1))
    half = share // halves
    chunks = [
        resident(last_kernel, array(half, groups, voxels, kb), ntm=ntm, skip=c * half)(residual, foot, t1_old, rx0, rx1)
        for c in range(halves)
    ]
    footprints_out = line_gather(chunks, "tm", ntm)

    pieces, origins = pair_gather(final, "pix", npix)
    traces_out = kernel(
        flip_kernel, (blocks // several,),
        [pl.BlockSpec((several, own, kb), lambda j: (j, 0, 0))] * npix,
        pl.BlockSpec((several, kb, frames), lambda j: (j, 0, 0)),
        array(blocks, kb, frames),
        scratch=[pltpu.VMEM((several, frames, kb), f32)], limit=LIMIT, origins=origins,
    )(*pieces)
    return footprints_out, traces_out


def solution(mesh):
    npix, ntm = mesh.shape["pix"], mesh.shape["tm"]
    in_specs = (
        P("pix", None, "tm"),
        P("pix", None, None, None),
        P(None, None, "tm"),
        P("pix", None),
        P(),
    )
    out_specs = (P("pix", None, None, None), P(None, None, "tm"))

    def body(*args):
        return local(*args, npix=npix, ntm=ntm)

    return jax.shard_map(body, mesh=mesh, in_specs=in_specs, out_specs=out_specs, check_vma=False)
```

```python
import functools

import jax
import jax.numpy as jnp
from jax import lax
from jax.experimental import pallas as pl
from jax.experimental.pallas import tpu as pltpu
from jax.sharding import PartitionSpec as P


EPSILON = 1e-06
LIMIT = 24 * 2**20
SUBLANES = 8
f32 = jnp.float32
bf16 = jnp.bfloat16


def up8(n):
    return -(-n // SUBLANES) * SUBLANES


def divisor(n, limits):
    return max(m for m in limits if n % m == 0)


def split(x):
    high = x.astype(bf16)
    return high, (x - high.astype(f32)).astype(bf16)


def dot(a, b, ca, cb):
    return lax.dot_general(a, b, (((ca,), (cb,)), ((), ())), preferred_element_type=f32)


def rows_by_rows(a, b):
    left = jnp.concatenate(a, axis=1)
    right = jnp.concatenate([b[0], b[0]], axis=1)
    return dot(left, right, 1, 1) + dot(a[0], b[1], 1, 1)


def rows_by_columns(a, b, ca=1):
    n = b[0].shape[1]
    both = dot(a[0], jnp.concatenate(b, axis=1), ca, 0)
    return both[:, :n] + both[:, n:] + dot(a[1], b[0], ca, 0)


def full_spec(shape):
    return pl.BlockSpec(shape, lambda *_: (0,) * len(shape))


def whole(space):
    return pl.BlockSpec(memory_space=space)


def squares(x):
    return jnp.sum(x * x, axis=0, keepdims=True)


def first_kernel(bl, y, foot, *refs, parts, own, step, extra):
    t0s, t1s = refs[:step], refs[step:2 * step]
    base_out, pay = refs[2 * step:]
    at = pl.program_id(0) * step
    count = bl.shape[0]
    kb = foot.shape[3]
    some = range(step)
    f0 = [split(foot[i, 0]) for i in some]
    f1 = [split(foot[i, 1]) for i in some]
    base = [y[i].astype(f32) - rows_by_columns(f1[i], split(t1s[i][0])) for i in some]
    residual = [split(base[i] - rows_by_columns(f0[i], split(t0s[i][0]))) for i in some]
    terms = [rows_by_columns(residual[i], f0[i], 0) for i in some]
    for i in some:
        base_out[i] = base[i]
        p = at + i
        pay[:, pl.ds(pl.multiple_of(p * own, SUBLANES), own), :] = terms[i].reshape(parts, own, kb)
        for g in range(2):
            norm = jnp.broadcast_to(squares(foot[i, g])[None], (parts, 1, kb))
            pay[:, pl.ds(count * own + g * count + p, 1), :] = norm

    @pl.when(at == 0)
    def _():
        shape = (extra, kb)
        where = lax.broadcasted_iota(jnp.int32, shape, 0) * kb + lax.broadcasted_iota(jnp.int32, shape, 1)
        listing = jnp.zeros(shape, jnp.int32)
        for p in range(count):
            for g in range(2):
                listing = jnp.where(where == 2 * p + g, bl[p, g], listing)
        pay[:, pay.shape[1] - extra:, :] = jnp.broadcast_to(listing.astype(f32)[None], (parts,) + shape)


def second_kernel(base, foot, rx, pay, *, parts, own, step):
    at = pl.program_id(0) * step
    kb = foot.shape[3]
    some = range(step)
    traces = [split(rx[:, i].reshape(parts * own, kb)) for i in some]
    residual = [split(base[i] - rows_by_rows(split(foot[i, 0]), traces[i])) for i in some]
    terms = [rows_by_columns(residual[i], split(foot[i, 1]), 0) for i in some]
    for i in some:
        pay[:, pl.ds(pl.multiple_of((at + i) * own, SUBLANES), own), :] = terms[i].reshape(parts, own, kb)


def prepare_kernel(order, pix, *refs, own, step):
    ins, out, flipped = refs[:step], refs[step], refs[step + 1]
    for i in range(step):
        flipped[i] = ins[i][0].T
        out[i] = flipped[i, pl.ds(pl.multiple_of(pix[0] * own, SUBLANES), own), :]


def owner_kernel(listing, place, order, rx, before, *refs, group, per, own, outs, outper, other):
    if other == "norms":
        after, back, norms1, totals, norms = refs
        norms1[...] = jnp.zeros(norms1.shape, f32)
        norms[...] = jnp.zeros(norms.shape, f32)
    else:
        norms, after, back, totals = refs
    sources = rx.shape[0]
    kb = rx.shape[2]
    bpg = before.shape[0]
    totals[...] = jnp.zeros(totals.shape, f32)

    @pl.loop(0, sources)
    def _(s):
        for i in range(per):
            p = s * per + i
            j = place[listing[p, group]] - group * bpg
            totals[j] = totals[j] + rx[s, i * own:(i + 1) * own, :]
            if other == "norms":
                row = per * own + i
                norms[j] = norms[j] + jnp.broadcast_to(rx[s, row:row + 1, :], (SUBLANES, kb))
                j1 = place[listing[p, 1]] - bpg
                row = per * own + per + i
                norms1[j1] = norms1[j1] + jnp.broadcast_to(rx[s, row:row + 1, :], (SUBLANES, kb))

    scale = kb * norms[:, 0:1, :] + EPSILON
    after[...] = jnp.maximum(before[...] + totals[...] / scale, 0.0)

    @pl.loop(0, outs)
    def _(s):
        for i in range(outper):
            j = place[listing[s * outper + i, group]] - group * bpg
            back[s, i * own:(i + 1) * own, :] = after[j]


def sort_kernel(order, after0, after1, final):
    bpg = after0.shape[0]

    @pl.loop(0, bpg, unroll=4)
    def _(j):
        final[order[j]] = after0[j]
        final[order[bpg + j]] = after1[j]


def owner(tables, rx, before, extra, *, group, per, outs, outper, other):
    bpg, own, kb = before.shape
    norms_shape = (bpg, SUBLANES, kb)
    shapes = [before.shape, (outs, outper * own, kb)]
    if other == "norms":
        shapes.append(norms_shape)
    scratch = [pltpu.VMEM(before.shape, f32)]
    if other == "norms":
        scratch.append(pltpu.VMEM(norms_shape, f32))
    return pl.pallas_call(
        functools.partial(owner_kernel, group=group, per=per, own=own, outs=outs, outper=outper, other=other),
        in_specs=[whole(pltpu.SMEM)] * 3 + [whole(pltpu.VMEM)] * (2 + len(extra)),
        out_specs=[whole(pltpu.VMEM)] * len(shapes),
        scratch_shapes=scratch,
        out_shape=[jax.ShapeDtypeStruct(shape, f32) for shape in shapes],
        compiler_params=pltpu.CompilerParams(vmem_limit_bytes=LIMIT),
        name="owner",
    )(*tables, rx, before, *extra)


def incoming(rx, i, me, ntm):
    pieces = []
    for s in range(ntm):
        piece = rx[:, lax.rem(me + (ntm - s), ntm), i]
        pieces.append(piece.reshape(piece.shape[0] * piece.shape[1], piece.shape[2]))
    return jnp.concatenate(pieces, axis=0)


def outgoing(pay, terms, p, me, ntm):
    npix, kb = pay.shape[0], terms.shape[1]
    own = terms.shape[0] // (npix * ntm)
    for s in range(ntm):
        piece = terms[s * npix * own:(s + 1) * npix * own].reshape(npix, own, kb)
        to = lax.rem(me + (ntm - s), ntm)
        pay[:, to, p * own:(p + 1) * own, :] = piece


def footprint_phase(residual, f0, f1, t0, t1):
    kb = f0[0].shape[1]
    s0, s1 = [split(t) for t in t0], [split(t) for t in t1]

    def renewed(residual, foot, trace, parts):
        weights = [rows_by_columns(split(r), s) for r, s in zip(residual, parts)]
        return [
            jnp.maximum(f + w / (kb * squares(t) + EPSILON), 0.0)
            for f, w, t in zip(foot, weights, trace)
        ]

    n0 = renewed(residual, f0, t0, s0)
    residual = [r - rows_by_rows(split(n - f), s) for r, n, f, s in zip(residual, n0, f0, s0)]
    n1 = renewed(residual, f1, t1, s1)
    return residual, n0, n1, s1


def third_kernel(*refs, ntm):
    ys, t0s = refs[:ntm], refs[ntm:2 * ntm]
    rx1, foot, residual_out, foot_out, t0_out, t1_out, pay = refs[2 * ntm:]
    me = lax.axis_index("tm")
    count, kb = foot.shape[0], foot.shape[3]
    own = (pay.shape[2] - up8(2 * count)) // count
    pair = divisor(count, (2, 1))
    for at in range(0, count, pair):
        some = range(at, at + pair)
        f0 = [foot[i, 0] for i in some]
        f1 = [foot[i, 1] for i in some]
        y = [jnp.concatenate([ref[i] for ref in ys], axis=1) for i in some]
        t0 = [
            jnp.concatenate([ref[:, i].reshape(ref.shape[0] * ref.shape[2], kb) for ref in t0s], axis=0)
            for i in some
        ]
        t1 = [incoming(rx1, i, me, ntm) for i in some]
        residual = [r - rows_by_rows(split(f), split(t)) for r, f, t in zip(y, f0, t0)]
        residual = [r - rows_by_rows(split(f), split(t)) for r, f, t in zip(residual, f1, t1)]
        residual, n0, n1, s1 = footprint_phase(residual, f0, f1, t0, t1)
        residual = [r - rows_by_rows(split(n - f), s) for r, n, f, s in zip(residual, n1, f1, s1)]
        terms = [rows_by_columns(split(r), split(n), 0) for r, n in zip(residual, n0)]
        for o, i in enumerate(some):
            residual_out[i] = residual[o]
            foot_out[i, 0] = n0[o]
            foot_out[i, 1] = n1[o]
            t0_out[i] = t0[o]
            t1_out[i] = t1[o]
            outgoing(pay, terms[o], i, me, ntm)
            for g, new in enumerate((n0[o], n1[o])):
                norm = jnp.broadcast_to(squares(new)[None, None], pay.shape[:2] + (1, kb))
                row = count * own + g * count + i
                pay[:, :, row:row + 1, :] = norm


def fourth_kernel(residual_in, foot, told, rx, residual_out, pay, *, ntm):
    me = lax.axis_index("tm")
    for i in range(told.shape[0]):
        change = incoming(rx, i, me, ntm) - told[i]
        residual = residual_in[i] - rows_by_rows(split(foot[i, 0]), split(change))
        residual_out[i] = residual
        outgoing(pay, rows_by_columns(split(residual), split(foot[i, 1]), 0), i, me, ntm)


def last_kernel(residual_in, foot, told, rx0, rx1, foot_out, *, ntm, skip):
    me = lax.axis_index("tm")
    some = range(skip, skip + foot_out.shape[0])
    f0 = [foot[i, 0] for i in some]
    f1 = [foot[i, 1] for i in some]
    t0 = [incoming(rx0, i, me, ntm) for i in some]
    t1 = [incoming(rx1, i, me, ntm) for i in some]
    residual = [
        residual_in[i] - rows_by_rows(split(f), split(t - told[i])) for i, f, t in zip(some, f1, t1)
    ]
    _, n0, n1, _ = footprint_phase(residual, f0, f1, t0, t1)
    for o in range(foot_out.shape[0]):
        foot_out[o, 0] = n0[o]
        foot_out[o, 1] = n1[o]


def flip_kernel(*refs, origins):
    pieces, out, frames = refs[:-2], refs[-2], refs[-1]
    count, own, _ = pieces[0].shape
    places = [pl.multiple_of(o * own, SUBLANES) for o in origins(lax.axis_index("pix"))]
    for j in range(count):
        for piece, place in zip(pieces, places):
            frames[j, pl.ds(place, own), :] = piece[j]
        out[j] = frames[j].T


def pair_gather(x, axis, n):
    chips = n // 2
    power = chips & (chips - 1) == 0

    def source(chip, s):
        return chip ^ s if power else lax.rem(chip + s, chips)

    def target(chip, s):
        return chip ^ s if power else (chip - s) % chips

    pieces = []
    for s in range(chips):
        perm = [(j, target(j // 2, s) * 2 + j % 2) for j in range(n)]
        pieces.append(lax.ppermute(x, axis, perm) if s else x)
    swap = [(j, j ^ 1) for j in range(n)]
    for s in range(chips):
        pieces.append(lax.ppermute(pieces[s], axis, swap))

    def origins(me):
        chip, core = me // 2, lax.rem(me, 2)
        return [source(chip, s) * 2 + c for c in (core, 1 - core) for s in range(chips)]

    return pieces, origins


def early_kernel(*refs, n, count, axis):
    chunks, rest, out, sems = refs[:count], refs[count:-2], refs[-2], refs[-1]
    me = lax.axis_index(axis)
    per = chunks[0].shape[0]
    from_left, from_right = rest[:(n - 2) * count], rest[(n - 2) * count:]

    def copy(source, s, c):
        place = lax.rem(me + s, n) * (count * per) + c * per
        return pltpu.make_async_copy(source, out.at[pl.ds(place, per)], sems.at[s, c])

    def every(act):
        for c in range(count):
            act(copy(chunks[c], 0, c))
            for s in range(1, n):
                if s <= n - 2:

                    @pl.when(me + s < n)
                    def _():
                        act(copy(from_right[(s - 1) * count + c], s, c))

                if s >= 2:

                    @pl.when(me + s >= n)
                    def _():
                        act(copy(from_left[(n - s - 1) * count + c], s, c))

    every(lambda one: one.start())
    every(lambda one: one.wait())


def ends_kernel(before, *refs, n, count, axis):
    from_left, from_right, out, sems = refs[:count], refs[count:2 * count], refs[-2], refs[-1]
    me = lax.axis_index(axis)
    per = from_left[0].shape[0]

    def move(sources, place):
        for c in range(count):
            pltpu.make_async_copy(
                sources[c], out.at[pl.ds((place * count + c) * per, per)], sems.at[c]
            ).start()
        for c in range(count):
            pltpu.make_async_copy(
                sources[c], out.at[pl.ds((place * count + c) * per, per)], sems.at[c]
            ).wait()

    @pl.when(me == 0)
    def _():
        move(from_right, n - 1)

    @pl.when(me == n - 1)
    def _():
        move(from_left, 0)


def line_gather(chunks, axis, n):
    size = sum(x.shape[0] for x in chunks)
    rest = chunks[0].shape[1:]
    left, right = list(chunks), list(chunks)
    from_left, from_right = {}, {}
    for s in range(1, n):
        for c in range(len(chunks)):
            left[c] = lax.ppermute(left[c], axis, [(j, j + 1) for j in range(n - 1)])
            right[c] = lax.ppermute(right[c], axis, [(j, j - 1) for j in range(1, n)])
            from_left[s, c], from_right[s, c] = left[c], right[c]
    shape = jax.ShapeDtypeStruct((n * size,) + rest, f32)
    early = [s for s in range(1, n - 1)]
    sources = list(chunks) + [d[s, c] for d in (from_left, from_right) for s in early for c in range(len(chunks))]
    out = pl.pallas_call(
        functools.partial(early_kernel, n=n, count=len(chunks), axis=axis),
        in_specs=[whole(pltpu.VMEM)] * len(sources),
        out_specs=whole(pltpu.HBM),
        out_shape=shape,
        scratch_shapes=[pltpu.SemaphoreType.DMA((n, len(chunks)))],
        compiler_params=pltpu.CompilerParams(vmem_limit_bytes=LIMIT),
        name="early",
    )(*sources)
    ends = [d[n - 1, c] for d in (from_left, from_right) for c in range(len(chunks))]
    return pl.pallas_call(
        functools.partial(ends_kernel, n=n, count=len(chunks), axis=axis),
        in_specs=[whole(pltpu.HBM)] + [whole(pltpu.VMEM)] * len(ends),
        out_specs=whole(pltpu.HBM),
        out_shape=shape,
        input_output_aliases={0: 0},
        scratch_shapes=[pltpu.SemaphoreType.DMA((len(chunks),))],
        compiler_params=pltpu.CompilerParams(vmem_limit_bytes=LIMIT),
        name="ends",
    )(out, *ends)


def local(recording, footprints, traces, block_list, block_order, *, npix, ntm):
    count, voxels, frames = recording.shape
    groups, kb = footprints.shape[1], footprints.shape[3]
    blocks = traces.shape[0]
    bpg = blocks // groups
    own = frames // npix
    share = count // ntm
    everyone = npix * ntm
    every = frames * ntm
    pix, tm = lax.axis_index("pix"), lax.axis_index("tm")
    me = jnp.reshape(tm, (1,)).astype(jnp.int32)

    def kernel(body, grid, in_specs, out_specs, out_shape, prefetch=0, scratch=(), limit=None, **static):
        return pl.pallas_call(
            functools.partial(body, **static),
            grid_spec=pltpu.PrefetchScalarGridSpec(
                num_scalar_prefetch=prefetch,
                grid=grid,
                in_specs=in_specs,
                out_specs=out_specs,
                scratch_shapes=scratch,
            ),
            out_shape=out_shape,
            compiler_params=pltpu.CompilerParams(vmem_limit_bytes=limit),
        )

    def resident(body, out_shape, **static):
        def run(*operands):
            return pl.pallas_call(
                functools.partial(body, **static),
                in_specs=[whole(pltpu.VMEM)] * len(operands),
                out_specs=jax.tree.map(lambda _: whole(pltpu.VMEM), out_shape),
                out_shape=out_shape,
                compiler_params=pltpu.CompilerParams(vmem_limit_bytes=LIMIT),
            )(*operands)

        return run

    def array(*shape):
        return jax.ShapeDtypeStruct(shape, f32)

    def exchange(x, axes):
        return lax.all_to_all(x, axes, 0, 0, tiled=True)

    y_pieces = []
    for s in range(ntm):
        to = lax.rem(tm + s, ntm)
        piece = lax.dynamic_slice_in_dim(recording, to * share, share, 0).astype(f32)
        y_pieces.append(lax.ppermute(piece, "tm", [(j, (j + s) % ntm) for j in range(ntm)]) if s else piece)

    pos_rows = up8(-(-count * groups // kb))
    place = jnp.zeros((blocks,), jnp.int32).at[block_order].set(jnp.arange(blocks, dtype=jnp.int32))

    step = divisor(count, (4, 2, 1))
    rows = count * own + up8(groups * count)
    foot_spec = pl.BlockSpec((step, groups, voxels, kb), lambda p, *_: (p, 0, 0, 0))
    patch_spec = pl.BlockSpec((step, voxels, frames), lambda p, *_: (p, 0, 0))

    def block_spec(i, g):
        return pl.BlockSpec((1, kb, frames), lambda p, bl: (bl[p * step + i, g], 0, 0))

    base, pay = kernel(
        first_kernel, (count // step,),
        [patch_spec, foot_spec] + [block_spec(i, g) for g in range(groups) for i in range(step)],
        [patch_spec, full_spec((npix, rows + pos_rows, kb))],
        [array(count, voxels, frames), array(npix, rows + pos_rows, kb)],
        prefetch=1, parts=npix, own=own, step=step, extra=pos_rows,
    )(block_list, recording, footprints, *[traces] * (groups * step))
    got = exchange(pay, "pix")

    several = divisor(bpg, (8, 4, 2, 1))
    whereabouts = jnp.reshape(pix, (1,)).astype(jnp.int32)

    def prepared(g):
        def ordered_spec(i):
            return pl.BlockSpec(
                (1, kb, frames), lambda b, order, pix: (order[g * bpg + b * several + i], 0, 0)
            )

        return kernel(
            prepare_kernel, (bpg // several,),
            [ordered_spec(i) for i in range(several)],
            pl.BlockSpec((several, own, kb), lambda b, *_: (b, 0, 0)),
            array(bpg, own, kb),
            prefetch=2, scratch=[pltpu.VMEM((several, frames, kb), f32)], own=own, step=several,
        )(block_order, whereabouts, *[traces] * several)

    before0, before1 = prepared(0), prepared(1)
    own_foot = lax.dynamic_slice_in_dim(footprints, tm * share, share, 0)

    listing = got[:, rows:, :].reshape(npix, -1)[:, :count * groups].reshape(npix * count, groups)
    tables = (listing.astype(jnp.int32), place, block_order)
    after0, back, norms1 = owner(
        tables, got, before0, (), group=0, per=count, outs=npix, outper=count, other="norms"
    )
    rx0 = exchange(back, "pix").reshape(npix, count, own, kb)

    t0_pieces = []
    for s in range(ntm):
        to = lax.rem(tm + s, ntm)
        piece = lax.dynamic_slice_in_dim(rx0, to * share, share, 1)
        t0_pieces.append(lax.ppermute(piece, "tm", [(j, (j + s) % ntm) for j in range(ntm)]) if s else piece)

    pay = kernel(
        second_kernel, (count // step,),
        [patch_spec, foot_spec, pl.BlockSpec((npix, step, own, kb), lambda p: (0, p, 0, 0))],
        full_spec((npix, count * own, kb)),
        array(npix, count * own, kb),
        parts=npix, own=own, step=step,
    )(base, footprints, rx0)
    after1, back = owner(
        tables, exchange(pay, "pix"), before1, (norms1,),
        group=1, per=count, outs=everyone, outper=share, other=None,
    )

    def spread(x):
        return exchange(x.reshape(everyone, x.shape[-2], kb), ("pix", "tm"))

    def landed(x):
        return x.reshape(npix, ntm, share, own, kb)

    rx1 = landed(spread(back))

    residual_type, trace_type = array(share, voxels, every), array(share, every, kb)
    wide = (npix, ntm, share * own + up8(groups * share), kb)
    narrow = (npix, ntm, share * own, kb)
    residual, foot, t0_old, t1_old, pay = resident(
        third_kernel, [residual_type, array(share, groups, voxels, kb), trace_type, trace_type, array(*wide)], ntm=ntm
    )(*y_pieces, *t0_pieces, rx1, own_foot)

    got = spread(pay)
    after0, back, norms1 = owner(
        tables, got, after0, (), group=0, per=share, outs=everyone, outper=share, other="norms"
    )
    rx0 = landed(spread(back))
    residual, pay = resident(fourth_kernel, [residual_type, array(*narrow)], ntm=ntm)(residual, foot, t0_old, rx0)
    got = spread(pay)
    after1, back = owner(
        tables, got, after1, (norms1,), group=1, per=share, outs=everyone, outper=share, other=None
    )
    rx1 = landed(spread(back))

    halves = divisor(share, (2, 1))
    half = share // halves
    chunks = [
        resident(last_kernel, array(half, groups, voxels, kb), ntm=ntm, skip=c * half)(residual, foot, t1_old, rx0, rx1)
        for c in range(halves)
    ]
    footprints_out = line_gather(chunks, "tm", ntm)

    final = pl.pallas_call(
        sort_kernel,
        in_specs=[whole(pltpu.SMEM), whole(pltpu.VMEM), whole(pltpu.VMEM)],
        out_specs=whole(pltpu.VMEM),
        out_shape=array(blocks, own, kb),
        compiler_params=pltpu.CompilerParams(vmem_limit_bytes=LIMIT),
        name="sort",
    )(block_order, after0, after1)
    pieces, origins = pair_gather(final, "pix", npix)
    traces_out = kernel(
        flip_kernel, (blocks // several,),
        [pl.BlockSpec((several, own, kb), lambda j: (j, 0, 0))] * npix,
        pl.BlockSpec((several, kb, frames), lambda j: (j, 0, 0)),
        array(blocks, kb, frames),
        scratch=[pltpu.VMEM((several, frames, kb), f32)], limit=LIMIT, origins=origins,
    )(*pieces)
    return footprints_out, traces_out


def solution(mesh):
    npix, ntm = mesh.shape["pix"], mesh.shape["tm"]
    in_specs = (
        P("pix", None, "tm"),
        P("pix", None, None, None),
        P(None, None, "tm"),
        P("pix", None),
        P(),
    )
    out_specs = (P("pix", None, None, None), P(None, None, "tm"))

    def body(*args):
        return local(*args, npix=npix, ntm=ntm)

    return jax.shard_map(body, mesh=mesh, in_specs=in_specs, out_specs=out_specs, check_vma=False)
```
